128 devices in a mesh: expert: 4 (over y_lo, core), shard: 32 (over z, y_hi, x).
Axes of the slice: x: 4, y: 4 (y_hi: 2, y_lo: 2; y = y_hi * 2 + y_lo), z: 4, core: 2. Of those that a mesh axis runs over, the one named last changes fastest.
Arguments:
- train_down: float32 [16, 6400, 4096], P('expert', None, 'shard'), may hold values from -0.15625 to 0.15625
- other_down: bfloat16 [16, 6400, 4096], P('expert', None, 'shard'), may hold values from -0.0390625 to 0.0390625
- router_weight: float32 [4096, 16], P('shard', 'expert'), may hold values from -0.09375 to 0.09375
- router_gain: float32 [4096], P('shard'), may hold values from 0.25 to 1.75
Outputs:
- ready_down: bfloat16 [16, 6400, 4096], P('expert', 'shard')
- scale_down: float32 [16, 6400], P('expert', 'shard')
- serve_router: bfloat16 [4096, 16], replicated
The draws below stay inside these ranges and needn't reach their ends.
All inputs are finite; a program needn't handle non-finite values.
Results may differ from the reference program's by a relative error of at most 0.001.
Values may be sent and summed in bfloat16 or wider, within the bound.
No kernel may reach another device: no remote copies, remote signals or barrier semaphores. Data moves between devices by JAX's collectives and lax.ppermute only.
A program may use at most 128 MiB of HBM per device.

```python
import jax
import jax.numpy as jnp
from jax import lax

EXPERTS = 16
D_MODEL = 4096
D_EXPERT = 6400


def with_spikes(array, rng, source, target, parts, factor):
    def block_of(axis_at):
        return (jnp.arange(array.shape[axis_at]) // (array.shape[axis_at] // parts)).reshape((-1,) + (1,) * (array.ndim - 1 - axis_at))

    first = jax.random.permutation(rng, parts)[block_of(target)]
    far = (block_of(target) + parts // 2) % parts
    return jnp.where((block_of(source) == first) | (block_of(source) == far), factor * array, array)


def block_levels(own_key, shape, cuts, low, high):
    gain = 1.0
    for axis_at, shards_of in cuts:
        steps = jax.random.uniform(jax.random.fold_in(jax.random.fold_in(own_key, 6), axis_at), (shards_of,), jnp.float32, low / len(cuts), high / len(cuts))
        gain = gain * jnp.repeat(jnp.exp(steps), shape[axis_at] // shards_of).reshape((-1,) + (1,) * (len(shape) - 1 - axis_at))
    return gain


def centred(rng, extent, deviation, bound, shards=(), held_as=jnp.bfloat16):
    result = jax.random.normal(rng, extent, jnp.float32) * deviation
    if len(shards) > 0:
        result = block_levels(rng, extent, shards, -0.22, 0.18) * result
    return jnp.clip(result, min=-bound, max=bound).astype(held_as)


def bell_draw_with(key, dims, deviation, reach, pieces, heavy, held_as=jnp.bfloat16):
    entries = deviation * jax.random.normal(key, dims, jnp.float32)
    if pieces:
        entries = entries * block_levels(key, dims, pieces, -0.22, 0.18)
    return jnp.clip(with_spikes(entries, jax.random.fold_in(key, 3), *heavy), -reach, reach).astype(held_as)


def setup_inputs(seed: int = 0) -> dict:
    key_of = jax.random.split(jax.random.key(seed), 5)
    return {
        "train_down": bell_draw_with(key_of[0], (EXPERTS, D_EXPERT, D_MODEL), D_EXPERT ** -0.5, 0.15625, ((0, 4), (2, 32)), (2, 1, 32, 2.75), jnp.float32),
        "other_down": centred(key_of[1], (EXPERTS, D_EXPERT, D_MODEL), (D_EXPERT * 4) ** -0.5, 0.0390625, ((0, 4), (2, 32))),
        "router_weight": centred(key_of[2], (D_MODEL, EXPERTS), D_MODEL ** -0.5, 0.09375, ((0, 32), (1, 4)), jnp.float32),
        "router_gain": jnp.clip(1.0 + 0.15 * jax.random.normal(key_of[3], (D_MODEL,), jnp.float32), 0.25, 1.75),
    }


def reference(train_down, other_down, router_weight, router_gain):
    latest_down = train_down + other_down.astype(jnp.float32)
    scale_down = jnp.sqrt(lax.optimization_barrier(jnp.sum(latest_down * latest_down, axis=2)))
    ready_down = (latest_down / jnp.expand_dims(scale_down, 2)).astype(jnp.bfloat16)
    serve_router = (router_weight * router_gain[:, None]).astype(jnp.bfloat16)
    return (ready_down, scale_down, serve_router)
```

```python
import functools

import jax
import jax.numpy as jnp
from jax import lax
from jax.experimental import pallas as pl
from jax.experimental.pallas import tpu as pltpu
from jax.sharding import PartitionSpec as P


LANES = 128
SPAN = 125.0
FLOOR = 1e-36


def encode_kernel(per, train_ref, other_ref, out_ref):
    experts, rows = train_ref.shape[0], train_ref.shape[1] // per
    tiles = rows // 8
    lane = lax.broadcasted_iota(jnp.int32, (8, LANES), 1)
    for p in range(per):
        peaks = jnp.zeros((8, LANES), jnp.float32)
        for e in range(experts):
            at = pl.ds(p * rows, rows)
            x = train_ref[e, at, :] + other_ref[e, at, :].astype(jnp.float32)
            peak = jnp.maximum(jnp.max(jnp.abs(x), axis=1, keepdims=True), FLOOR)
            peak = peak.astype(jnp.bfloat16).astype(jnp.float32)
            code = jnp.exp2(x * (SPAN / peak))
            out_ref[p, e * rows : (e + 1) * rows, :] = code.astype(jnp.bfloat16)
            for k in range(tiles):
                peaks = jnp.where(lane == e * tiles + k, peak[8 * k : 8 * k + 8], peaks)
        out_ref[p, experts * rows :, :] = peaks.astype(jnp.bfloat16)


def encode(train, other, parts, per=1):
    experts, length, _ = train.shape
    rows = length // parts
    height = experts * rows + 8
    block = pl.BlockSpec((experts, per * rows, LANES), lambda d: (0, d, 0))
    return pl.pallas_call(
        functools.partial(encode_kernel, per),
        grid=(parts // per,),
        in_specs=[block, block],
        out_specs=pl.BlockSpec((per, height, LANES), lambda d: (d, 0, 0)),
        out_shape=jax.ShapeDtypeStruct((parts, height, LANES), jnp.bfloat16),
        name="encode",
    )(train, other)


def decode_kernel(code_ref, ready_ref, scale_ref, value_ref, total_ref, wide_ref, sems):
    parts = code_ref.shape[0]
    experts, rows = scale_ref.shape
    tiles = rows // 8
    count = experts * tiles

    total_ref[...] = jnp.zeros(total_ref.shape, jnp.float32)

    def take(s, carry):
        peaks = code_ref[s, 8 * count :, :].astype(jnp.float32) * (1.0 / SPAN)
        for k in range(0, count, 2):
            code = code_ref[s, 8 * k : 8 * k + 16, :].astype(jnp.float32)
            power = jnp.log2(code)
            for h in range(2):
                at = pl.ds(8 * (k + h), 8)
                value = power[8 * h : 8 * h + 8] * peaks[:, k + h : k + h + 1]
                value_ref[s, at, :] = value
                total_ref[at, :] += value * value
        return carry

    lax.fori_loop(0, parts, take, 0)

    lane = lax.broadcasted_iota(jnp.int32, (8, LANES), 1)
    row = lax.broadcasted_iota(jnp.int32, (8, LANES), 0)
    for e in range(experts):
        for first in range(0, tiles, 16):
            line = jnp.zeros((8, LANES), jnp.float32)
            last = min(first + 16, tiles)
            for j in range(first, last):
                at = pl.ds(8 * (e * tiles + j), 8)
                scale = jnp.sqrt(jnp.sum(total_ref[at, :], axis=1, keepdims=True))
                line = jnp.where(lane - row == 8 * (j - first), scale, line)
                total_ref[at, :] = jnp.broadcast_to(1.0 / scale, (8, LANES))
            width = 8 * (last - first)
            scale_ref[e : e + 1, 8 * first : 8 * last] = jnp.sum(line, axis=0, keepdims=True)[:, :width]

    def copy_of(e):
        return pltpu.make_async_copy(wide_ref.at[e], ready_ref.at[e], sems.at[e])

    for e in range(experts):

        def give(s, carry):
            for j in range(tiles):
                at = pl.ds(8 * (e * tiles + j), 8)
                value = value_ref[s, at, :] * total_ref[at, :]
                wide_ref[e, 8 * j : 8 * j + 8, pl.ds(pl.multiple_of(s * LANES, LANES), LANES)] = value.astype(jnp.bfloat16)
            return carry

        lax.fori_loop(0, parts, give, 0)
        copy_of(e).start()
    for e in range(experts):
        copy_of(e).wait()


def decode(code, experts, rows):
    parts, height, _ = code.shape
    return pl.pallas_call(
        decode_kernel,
        in_specs=[pl.BlockSpec(memory_space=pltpu.VMEM)],
        out_specs=[pl.BlockSpec(memory_space=pl.ANY), pl.BlockSpec(memory_space=pltpu.VMEM)],
        out_shape=[
            jax.ShapeDtypeStruct((experts, rows, parts * LANES), jnp.bfloat16),
            jax.ShapeDtypeStruct((experts, rows), jnp.float32),
        ],
        scratch_shapes=[
            pltpu.VMEM((parts, experts * rows, LANES), jnp.float32),
            pltpu.VMEM((experts * rows, LANES), jnp.float32),
            pltpu.VMEM((experts, rows, parts * LANES), jnp.bfloat16),
            pltpu.SemaphoreType.DMA((experts,)),
        ],
        name="decode",
    )(code)


def doubled(x, axis, bit, dim):
    pairs = [(i, i ^ bit) for i in range(lax.axis_size(axis))]
    got = lax.ppermute(x, axis, pairs)
    second = (lax.axis_index(axis) & bit) != 0
    return jnp.concatenate([jnp.where(second, got, x), jnp.where(second, x, got)], axis=dim)


def per_device(train_down, other_down, router_weight, router_gain):
    parts = lax.axis_size("shard")
    experts, length, _ = train_down.shape
    sent = encode(train_down, other_down, parts)
    code = lax.all_to_all(sent, "shard", 0, 0, tiled=True)
    router = (router_weight * router_gain[:, None]).astype(jnp.bfloat16).T
    for axis, dim in (("shard", 1), ("expert", 0)):
        bit = 1
        while bit < lax.axis_size(axis):
            router = doubled(router, axis, bit, dim)
            bit *= 2
    ready_down, scale_down = decode(code, experts, length // parts)
    return (ready_down, scale_down, router.T)


def solution(mesh):
    in_specs = (
        P("expert", None, "shard"),
        P("expert", None, "shard"),
        P("shard", "expert"),
        P("shard"),
    )
    out_specs = (P("expert", "shard", None), P("expert", "shard"), P())
    return jax.shard_map(
        per_device, mesh=mesh, in_specs=in_specs, out_specs=out_specs, check_vma=False
    )
```

```python
import jax
import jax.numpy as jnp
from jax import lax
from jax.experimental import pallas as pl
from jax.experimental.pallas import tpu as pltpu
from jax.sharding import PartitionSpec as P


LANES = 128
SPAN = 125.0
FLOOR = 1e-36
PAIR = 8


def encode_kernel(train_ref, other_ref, out_ref, train_buf, other_buf, train_sems, other_sems):
    parts, experts, rows, _ = train_buf.shape
    tiles = rows // 8
    place = lax.broadcasted_iota(jnp.int32, (8, LANES), 1) - lax.broadcasted_iota(jnp.int32, (8, LANES), 0)

    def train_copy(d):
        return pltpu.make_async_copy(train_ref.at[:, pl.ds(d * rows, rows), :], train_buf.at[d], train_sems.at[d])

    def other_copy(d):
        return pltpu.make_async_copy(other_ref.at[:, pl.ds(d * rows, rows), :], other_buf.at[d], other_sems.at[d])

    for d in range(parts):
        train_copy(d).start()
        other_copy(d).start()

    def step(d, carry):
        train_copy(d).wait()
        other_copy(d).wait()
        peaks = []
        for e in range(experts):
            x = train_buf[d, e] + other_buf[d, e].astype(jnp.float32)
            peak = jnp.maximum(jnp.max(jnp.abs(x), axis=1, keepdims=True), FLOOR)
            peak = peak.astype(jnp.bfloat16).astype(jnp.float32)
            code = jnp.exp2(x * (SPAN / peak))
            out_ref[d, e * rows : (e + 1) * rows, :] = code.astype(jnp.bfloat16)
            for first in (0, 16):
                line = jnp.zeros((8, LANES), jnp.float32)
                for k in range(first, min(first + 16, tiles)):
                    line = jnp.where(place == 8 * (k - first), peak[8 * k : 8 * k + 8], line)
                peaks.append(jnp.sum(line, axis=0, keepdims=True))
        out_ref[d, experts * rows : experts * rows + 8, :] = jnp.concatenate(peaks).astype(jnp.bfloat16)
        return carry

    lax.fori_loop(0, parts, step, 0)


def encode(train, other, parts, height):
    experts, length, _ = train.shape
    rows = length // parts
    hbm = pl.BlockSpec(memory_space=pltpu.HBM)
    return pl.pallas_call(
        encode_kernel,
        in_specs=[hbm, hbm],
        out_specs=pl.BlockSpec(memory_space=pltpu.VMEM),
        out_shape=pltpu.VMEM((parts, height, LANES), jnp.bfloat16),
        scratch_shapes=[
            pltpu.VMEM((parts, experts, rows, LANES), jnp.float32),
            pltpu.VMEM((parts, experts, rows, LANES), jnp.bfloat16),
            pltpu.SemaphoreType.DMA((parts,)),
            pltpu.SemaphoreType.DMA((parts,)),
        ],
        compiler_params=pltpu.CompilerParams(vmem_limit_bytes=22 * 2**20),
        name="encode",
    )(pltpu.with_memory_space_constraint(train, pltpu.HBM), pltpu.with_memory_space_constraint(other, pltpu.HBM))


def router_kernel(sent_ref, gain_ref, w0, w1, w2, w3, out_ref):
    parts, height, _ = out_ref.shape
    mine = lax.axis_index("expert")
    low = jnp.concatenate([w0[...], w1[...]]) * gain_ref[...]
    high = jnp.concatenate([w2[...], w3[...]]) * gain_ref[...]
    low, high = [jnp.where(mine & 1 != 0, pltpu.roll(x, 4, 0), x) for x in (low, high)]
    low, high = jnp.where(mine & 2 != 0, high, low), jnp.where(mine & 2 != 0, low, high)
    both = jnp.concatenate([low, high]).astype(jnp.bfloat16)
    for d in range(parts):
        out_ref[d, height - 16 :, :] = both


def with_router(sent, gain, weights):
    vmem = pl.BlockSpec(memory_space=pltpu.VMEM)
    return pl.pallas_call(
        router_kernel,
        in_specs=[vmem] * (2 + len(weights)),
        out_specs=vmem,
        out_shape=pltpu.VMEM(sent.shape, sent.dtype),
        input_output_aliases={0: 0},
        compiler_params=pltpu.CompilerParams(vmem_limit_bytes=2 * 2**20),
        name="router",
    )(pltpu.with_memory_space_constraint(sent, pltpu.VMEM), gain, *weights)


def decode_kernel(
    code_ref, ready_ref, scale_ref, router_ref, peak_buf, even_buf, odd_buf, even_root, odd_root, wide_buf, scale_buf, router_buf, sems
):
    parts = code_ref.shape[0]
    experts, rows, _ = wide_buf.shape
    tiles = rows // 8
    total = experts * rows
    steps = parts // PAIR

    def wide_copy(e):
        return pltpu.make_async_copy(wide_buf.at[e], ready_ref.at[e], sems.at[e])

    scale_copy = pltpu.make_async_copy(scale_buf, scale_ref, sems.at[experts])
    router_copy = pltpu.make_async_copy(router_buf, router_ref, sems.at[experts + 1])

    for s in range(parts):
        router_buf[:, s * LANES : (s + 1) * LANES] = code_ref[s, total + 8 :, :]
        peak_buf[s] = code_ref[s, total : total + 8, :].astype(jnp.float32)
    router_copy.start()

    source = lax.broadcasted_iota(jnp.int32, (parts, PAIR * LANES), 0)
    column = lax.broadcasted_iota(jnp.int32, (parts, PAIR * LANES), 1) // LANES

    def take(e, step, peaks, values, squares):
        first = step * PAIR
        spread = jnp.where(source == column + first, 1.0, 0.0).astype(jnp.bfloat16)
        peak = jnp.dot(peaks, spread, preferred_element_type=jnp.float32)
        for u in range(PAIR):
            code = code_ref[first + u, e * rows : (e + 1) * rows, :].astype(jnp.float32)
            value = jnp.log2(code) * peak[:, u * LANES : (u + 1) * LANES]
            values[first + u] = value
            squares = squares + value * value
        return squares

    def give(e, step, values, roots):
        for u in range(PAIR):
            s = step * PAIR + u
            at = pl.ds(pl.multiple_of(s * LANES, LANES), LANES)
            wide_buf[e, :, at] = (values[s] * roots[...]).astype(jnp.bfloat16)

    lane = lax.broadcasted_iota(jnp.int32, (8, LANES), 1)
    row = lax.broadcasted_iota(jnp.int32, (8, LANES), 0)
    buffers = ((even_buf, even_root), (odd_buf, odd_root))
    for e in range(experts + 1):
        values, roots = buffers[e % 2]
        old_values, old_roots = buffers[1 - e % 2]
        if e < experts:
            peaks = jnp.concatenate([peak_buf[:, 2 * e, :], peak_buf[:, 2 * e + 1, :]], axis=1)
            peaks = peaks.T[:rows].astype(jnp.bfloat16)

        def step(i, squares):
            if e < experts:
                squares = take(e, i, peaks, values, squares)
            if e > 0:
                give(e - 1, i, old_values, old_roots)
            return squares

        squares = lax.fori_loop(0, steps, step, jnp.zeros((rows, LANES), jnp.float32))
        if e > 0:
            wide_copy(e - 1).start()
        if e < experts:
            square = jnp.sum(squares, axis=1, keepdims=True)
            root = lax.rsqrt(square)
            roots[...] = jnp.broadcast_to(root, (rows, LANES))
            scale = square * root * (1.0 / SPAN)
            for first in range(0, tiles, 16):
                line = jnp.zeros((8, LANES), jnp.float32)
                last = min(first + 16, tiles)
                for j in range(first, last):
                    line = jnp.where(lane - row == 8 * (j - first), scale[8 * j : 8 * j + 8], line)
                width = 8 * (last - first)
                scale_buf[e : e + 1, 8 * first : 8 * last] = jnp.sum(line, axis=0, keepdims=True)[:, :width]
        if e == experts - 1:
            scale_copy.start()
    router_copy.wait()
    scale_copy.wait()
    for e in range(experts):
        wide_copy(e).wait()


def decode(code, experts, rows):
    parts, height, _ = code.shape
    total = experts * rows
    hbm = pl.BlockSpec(memory_space=pltpu.HBM)
    tail = height - total - 8
    return pl.pallas_call(
        decode_kernel,
        in_specs=[pl.BlockSpec(memory_space=pltpu.VMEM)],
        out_specs=[hbm] * 3,
        out_shape=[
            jax.ShapeDtypeStruct((experts, rows, parts * LANES), jnp.bfloat16),
            jax.ShapeDtypeStruct((experts, rows), jnp.float32),
            jax.ShapeDtypeStruct((tail, parts * LANES), jnp.bfloat16),
        ],
        scratch_shapes=[
            pltpu.VMEM((parts, 8, LANES), jnp.float32),
            pltpu.VMEM((parts, rows, LANES), jnp.float32),
            pltpu.VMEM((parts, rows, LANES), jnp.float32),
            pltpu.VMEM((rows, LANES), jnp.float32),
            pltpu.VMEM((rows, LANES), jnp.float32),
            pltpu.VMEM((experts, rows, parts * LANES), jnp.bfloat16),
            pltpu.VMEM((experts, rows), jnp.float32),
            pltpu.VMEM((tail, parts * LANES), jnp.bfloat16),
            pltpu.SemaphoreType.DMA((experts + 2,)),
        ],
        compiler_params=pltpu.CompilerParams(vmem_limit_bytes=20 * 2**20),
        name="decode",
    )(pltpu.with_memory_space_constraint(code, pltpu.VMEM))


def of_all_experts(x):
    count = lax.axis_size("expert")
    return [x] + [lax.ppermute(x, "expert", [(i, i ^ j) for i in range(count)]) for j in range(1, count)]


def per_device(train_down, other_down, router_weight, router_gain):
    parts = lax.axis_size("shard")
    experts, length, _ = train_down.shape
    rows = length // parts
    weights = of_all_experts(router_weight.T)
    sent = encode(train_down, other_down, parts, experts * rows + 24)
    sent = with_router(sent, router_gain[None], weights)
    code = lax.all_to_all(sent, "shard", 0, 0, tiled=True)
    ready_down, scale_down, serve_router = decode(code, experts, rows)
    return (ready_down, scale_down, serve_router.T)


def solution(mesh):
    in_specs = (
        P("expert", None, "shard"),
        P("expert", None, "shard"),
        P("shard", "expert"),
        P("shard"),
    )
    out_specs = (P("expert", "shard", None), P("expert", "shard"), P())
    return jax.shard_map(
        per_device, mesh=mesh, in_specs=in_specs, out_specs=out_specs, check_vma=False
    )
```

```python
import jax
import jax.numpy as jnp
from jax import lax
from jax.experimental import pallas as pl
from jax.experimental.pallas import tpu as pltpu
from jax.sharding import PartitionSpec as P


LANES = 128
SPAN = 125.0
FLOOR = 1e-36
PAIR = 32
TOGETHER = 2


def encode_kernel(train_ref, other_ref, out_ref, train_buf, other_buf, train_sems, other_sems):
    parts, experts, rows, _ = train_buf.shape
    tiles = rows // 8
    place = lax.broadcasted_iota(jnp.int32, (8, LANES), 1) - lax.broadcasted_iota(jnp.int32, (8, LANES), 0)

    def train_copy(d):
        return pltpu.make_async_copy(train_ref.at[:, pl.ds(d * rows, rows), :], train_buf.at[d], train_sems.at[d])

    def other_copy(d):
        return pltpu.make_async_copy(other_ref.at[:, pl.ds(d * rows, rows), :], other_buf.at[d], other_sems.at[d])

    for d in range(parts):
        train_copy(d).start()
        other_copy(d).start()

    def code_of(d):
        peaks = []
        for e in range(0, experts, 2):
            x = jnp.concatenate([train_buf[d, e + h] + other_buf[d, e + h].astype(jnp.float32) for h in range(2)])
            peak = jnp.max(jnp.abs(x.astype(jnp.bfloat16)), axis=1, keepdims=True)
            peak = jnp.maximum(peak, jnp.bfloat16(FLOOR)).astype(jnp.float32)
            code = jnp.exp2(x * (SPAN / peak))
            out_ref[d, e * rows : (e + 2) * rows, :] = code.astype(jnp.bfloat16)
            for h in range(2):
                for first in (0, 16):
                    line = jnp.zeros((8, LANES), jnp.float32)
                    for k in range(first, min(first + 16, tiles)):
                        at = h * rows + 8 * k
                        line = jnp.where(place == 8 * (k - first), peak[at : at + 8], line)
                    peaks.append(jnp.sum(line, axis=0, keepdims=True))
        out_ref[d, experts * rows : experts * rows + 8, :] = jnp.concatenate(peaks).astype(jnp.bfloat16)

    def step(i, carry):
        for u in range(TOGETHER):
            train_copy(i * TOGETHER + u).wait()
            other_copy(i * TOGETHER + u).wait()
        for u in range(TOGETHER):
            code_of(i * TOGETHER + u)
        return carry

    lax.fori_loop(0, parts // TOGETHER, step, 0)


def encode(train, other, parts, height):
    experts, length, _ = train.shape
    rows = length // parts
    hbm = pl.BlockSpec(memory_space=pltpu.HBM)
    return pl.pallas_call(
        encode_kernel,
        in_specs=[hbm, hbm],
        out_specs=pl.BlockSpec(memory_space=pltpu.VMEM),
        out_shape=pltpu.VMEM((parts, height, LANES), jnp.bfloat16),
        scratch_shapes=[
            pltpu.VMEM((parts, experts, rows, LANES), jnp.float32),
            pltpu.VMEM((parts, experts, rows, LANES), jnp.bfloat16),
            pltpu.SemaphoreType.DMA((parts,)),
            pltpu.SemaphoreType.DMA((parts,)),
        ],
        compiler_params=pltpu.CompilerParams(vmem_limit_bytes=22 * 2**20),
        name="encode",
    )(pltpu.with_memory_space_constraint(train, pltpu.HBM), pltpu.with_memory_space_constraint(other, pltpu.HBM))


def router_kernel(sent_ref, gain_ref, w0, w1, w2, w3, out_ref):
    parts, height, _ = out_ref.shape
    mine = lax.axis_index("expert")
    low = jnp.concatenate([w0[...], w1[...]]) * gain_ref[...]
    high = jnp.concatenate([w2[...], w3[...]]) * gain_ref[...]
    low, high = [jnp.where(mine & 1 != 0, pltpu.roll(x, 4, 0), x) for x in (low, high)]
    low, high = jnp.where(mine & 2 != 0, high, low), jnp.where(mine & 2 != 0, low, high)
    both = jnp.concatenate([low, high]).astype(jnp.bfloat16)
    for d in range(parts):
        out_ref[d, height - 16 :, :] = both


def with_router(sent, gain, weights):
    vmem = pl.BlockSpec(memory_space=pltpu.VMEM)
    return pl.pallas_call(
        router_kernel,
        in_specs=[vmem] * (2 + len(weights)),
        out_specs=vmem,
        out_shape=pltpu.VMEM(sent.shape, sent.dtype),
        input_output_aliases={0: 0},
        compiler_params=pltpu.CompilerParams(vmem_limit_bytes=2 * 2**20),
        name="router",
    )(pltpu.with_memory_space_constraint(sent, pltpu.VMEM), gain, *weights)


def decode_kernel(
    code_ref, ready_ref, scale_ref, router_ref, peak_buf, even_buf, odd_buf, even_root, odd_root, wide_buf, scale_buf, router_buf, sems
):
    parts = code_ref.shape[0]
    experts, rows, _ = wide_buf.shape
    tiles = rows // 8
    total = experts * rows
    steps = parts // PAIR

    def wide_copy(e):
        return pltpu.make_async_copy(wide_buf.at[e], ready_ref.at[e], sems.at[e])

    scale_copy = pltpu.make_async_copy(scale_buf, scale_ref, sems.at[experts])
    router_copy = pltpu.make_async_copy(router_buf, router_ref, sems.at[experts + 1])

    for s in range(parts):
        router_buf[:, s * LANES : (s + 1) * LANES] = code_ref[s, total + 8 :, :]
        peak_buf[s] = code_ref[s, total : total + 8, :].astype(jnp.float32)
    router_copy.start()

    source = lax.broadcasted_iota(jnp.int32, (parts, PAIR * LANES), 0)
    column = lax.broadcasted_iota(jnp.int32, (parts, PAIR * LANES), 1) // LANES

    def take(e, step, peaks, values, squares):
        first = step * PAIR
        spread = jnp.where(source == column + first, 1.0, 0.0).astype(jnp.bfloat16)
        peak = jnp.dot(peaks, spread, preferred_element_type=jnp.float32)
        for u in range(PAIR):
            code = code_ref[first + u, e * rows : (e + 1) * rows, :].astype(jnp.float32)
            value = jnp.log2(code) * peak[:, u * LANES : (u + 1) * LANES]
            values[first + u] = value
            squares = squares + value * value
        return squares

    def give(e, step, values, roots):
        for u in range(PAIR):
            s = step * PAIR + u
            at = pl.ds(pl.multiple_of(s * LANES, LANES), LANES)
            wide_buf[e, :, at] = (values[s] * roots[...]).astype(jnp.bfloat16)

    lane = lax.broadcasted_iota(jnp.int32, (8, LANES), 1)
    row = lax.broadcasted_iota(jnp.int32, (8, LANES), 0)
    buffers = ((even_buf, even_root), (odd_buf, odd_root))
    for e in range(experts + 1):
        values, roots = buffers[e % 2]
        old_values, old_roots = buffers[1 - e % 2]
        if e < experts:
            peaks = jnp.concatenate([peak_buf[:, 2 * e, :], peak_buf[:, 2 * e + 1, :]], axis=1)
            peaks = peaks.T[:rows].astype(jnp.bfloat16)

        def step(i, squares):
            if e < experts:
                squares = take(e, i, peaks, values, squares)
            if e > 0:
                give(e - 1, i, old_values, old_roots)
            return squares

        squares = lax.fori_loop(0, steps, step, jnp.zeros((rows, LANES), jnp.float32))
        if e > 0:
            wide_copy(e - 1).start()
        if e < experts:
            square = jnp.sum(squares, axis=1, keepdims=True)
            root = lax.rsqrt(square)
            roots[...] = jnp.broadcast_to(root, (rows, LANES))
            scale = square * root * (1.0 / SPAN)
            for first in range(0, tiles, 16):
                line = jnp.zeros((8, LANES), jnp.float32)
                last = min(first + 16, tiles)
                for j in range(first, last):
                    line = jnp.where(lane - row == 8 * (j - first), scale[8 * j : 8 * j + 8], line)
                width = 8 * (last - first)
                scale_buf[e : e + 1, 8 * first : 8 * last] = jnp.sum(line, axis=0, keepdims=True)[:, :width]
        if e == experts - 1:
            scale_copy.start()
    router_copy.wait()
    scale_copy.wait()
    for e in range(experts):
        wide_copy(e).wait()


def decode(code, experts, rows):
    parts, height, _ = code.shape
    total = experts * rows
    hbm = pl.BlockSpec(memory_space=pltpu.HBM)
    tail = height - total - 8
    return pl.pallas_call(
        decode_kernel,
        in_specs=[pl.BlockSpec(memory_space=pltpu.VMEM)],
        out_specs=[hbm] * 3,
        out_shape=[
            jax.ShapeDtypeStruct((experts, rows, parts * LANES), jnp.bfloat16),
            jax.ShapeDtypeStruct((experts, rows), jnp.float32),
            jax.ShapeDtypeStruct((tail, parts * LANES), jnp.bfloat16),
        ],
        scratch_shapes=[
            pltpu.VMEM((parts, 8, LANES), jnp.float32),
            pltpu.VMEM((parts, rows, LANES), jnp.float32),
            pltpu.VMEM((parts, rows, LANES), jnp.float32),
            pltpu.VMEM((rows, LANES), jnp.float32),
            pltpu.VMEM((rows, LANES), jnp.float32),
            pltpu.VMEM((experts, rows, parts * LANES), jnp.bfloat16),
            pltpu.VMEM((experts, rows), jnp.float32),
            pltpu.VMEM((tail, parts * LANES), jnp.bfloat16),
            pltpu.SemaphoreType.DMA((experts + 2,)),
        ],
        compiler_params=pltpu.CompilerParams(vmem_limit_bytes=20 * 2**20),
        name="decode",
    )(pltpu.with_memory_space_constraint(code, pltpu.VMEM))


def of_all_experts(x):
    count = lax.axis_size("expert")
    return [x] + [lax.ppermute(x, "expert", [(i, i ^ j) for i in range(count)]) for j in range(1, count)]


def per_device(train_down, other_down, router_weight, router_gain):
    parts = lax.axis_size("shard")
    experts, length, _ = train_down.shape
    rows = length // parts
    weights = of_all_experts(router_weight.T)
    sent = encode(train_down, other_down, parts, experts * rows + 24)
    sent = with_router(sent, router_gain[None], weights)
    code = lax.all_to_all(sent, "shard", 0, 0, tiled=True)
    ready_down, scale_down, serve_router = decode(code, experts, rows)
    return (ready_down, scale_down, serve_router.T)


def solution(mesh):
    in_specs = (
        P("expert", None, "shard"),
        P("expert", None, "shard"),
        P("shard", "expert"),
        P("shard"),
    )
    out_specs = (P("expert", "shard", None), P("expert", "shard"), P())
    return jax.shard_map(
        per_device, mesh=mesh, in_specs=in_specs, out_specs=out_specs, check_vma=False
    )
```

```python
import jax
import jax.numpy as jnp
from jax import lax
from jax.experimental import pallas as pl
from jax.experimental.pallas import tpu as pltpu
from jax.sharding import PartitionSpec as P


LANES = 128
SPAN = 125.0
FLOOR = 1e-36
PAIR = 32
TOGETHER = 2


def encode_kernel(train_ref, other_ref, out_ref, train_buf, other_buf, train_sems, other_sems):
    turns, experts, rows, _ = train_buf.shape
    parts, rows = turns * TOGETHER, rows // TOGETHER
    tiles = rows // 8
    place = lax.broadcasted_iota(jnp.int32, (8, LANES), 1) - lax.broadcasted_iota(jnp.int32, (8, LANES), 0)

    def train_copy(d):
        return pltpu.make_async_copy(train_ref.at[:, pl.ds(d * TOGETHER * rows, TOGETHER * rows), :], train_buf.at[d], train_sems.at[d])

    def other_copy(d):
        return pltpu.make_async_copy(other_ref.at[:, pl.ds(d * TOGETHER * rows, TOGETHER * rows), :], other_buf.at[d], other_sems.at[d])

    for d in range(turns):
        train_copy(d).start()
        other_copy(d).start()

    def code_of(i, u):
        d = i * TOGETHER + u
        near = slice(u * rows, (u + 1) * rows)
        peaks = []
        for e in range(0, experts, 2):
            x = jnp.concatenate([train_buf[i, e + h, near] + other_buf[i, e + h, near].astype(jnp.float32) for h in range(2)])
            peak = jnp.max(jnp.abs(x.astype(jnp.bfloat16)), axis=1, keepdims=True)
            peak = jnp.maximum(peak, jnp.bfloat16(FLOOR)).astype(jnp.float32)
            code = jnp.exp2(x * (SPAN / peak))
            out_ref[d, e * rows : (e + 2) * rows, :] = code.astype(jnp.bfloat16)
            for h in range(2):
                for first in (0, 16):
                    line = jnp.zeros((8, LANES), jnp.float32)
                    for k in range(first, min(first + 16, tiles)):
                        at = h * rows + 8 * k
                        line = jnp.where(place == 8 * (k - first), peak[at : at + 8], line)
                    peaks.append(jnp.sum(line, axis=0, keepdims=True))
        out_ref[d, experts * rows : experts * rows + 8, :] = jnp.concatenate(peaks).astype(jnp.bfloat16)

    def step(i, carry):
        train_copy(i).wait()
        other_copy(i).wait()
        for u in range(TOGETHER):
            code_of(i, u)
        return carry

    lax.fori_loop(0, turns, step, 0)


def encode(train, other, parts, height):
    experts, length, _ = train.shape
    rows = length // parts
    hbm = pl.BlockSpec(memory_space=pltpu.HBM)
    return pl.pallas_call(
        encode_kernel,
        in_specs=[hbm, hbm],
        out_specs=pl.BlockSpec(memory_space=pltpu.VMEM),
        out_shape=pltpu.VMEM((parts, height, LANES), jnp.bfloat16),
        scratch_shapes=[
            pltpu.VMEM((parts // TOGETHER, experts, TOGETHER * rows, LANES), jnp.float32),
            pltpu.VMEM((parts // TOGETHER, experts, TOGETHER * rows, LANES), jnp.bfloat16),
            pltpu.SemaphoreType.DMA((parts // TOGETHER,)),
            pltpu.SemaphoreType.DMA((parts // TOGETHER,)),
        ],
        compiler_params=pltpu.CompilerParams(vmem_limit_bytes=22 * 2**20),
        name="encode",
    )(pltpu.with_memory_space_constraint(train, pltpu.HBM), pltpu.with_memory_space_constraint(other, pltpu.HBM))


def router_kernel(sent_ref, gain_ref, w0, w1, w2, w3, out_ref):
    parts, height, _ = out_ref.shape
    mine = lax.axis_index("expert")
    low = jnp.concatenate([w0[...], w1[...]]) * gain_ref[...]
    high = jnp.concatenate([w2[...], w3[...]]) * gain_ref[...]
    low, high = [jnp.where(mine & 1 != 0, pltpu.roll(x, 4, 0), x) for x in (low, high)]
    low, high = jnp.where(mine & 2 != 0, high, low), jnp.where(mine & 2 != 0, low, high)
    both = jnp.concatenate([low, high]).astype(jnp.bfloat16)
    for d in range(parts):
        out_ref[d, height - 16 :, :] = both


def with_router(sent, gain, weights):
    vmem = pl.BlockSpec(memory_space=pltpu.VMEM)
    return pl.pallas_call(
        router_kernel,
        in_specs=[vmem] * (2 + len(weights)),
        out_specs=vmem,
        out_shape=pltpu.VMEM(sent.shape, sent.dtype),
        input_output_aliases={0: 0},
        compiler_params=pltpu.CompilerParams(vmem_limit_bytes=2 * 2**20),
        name="router",
    )(pltpu.with_memory_space_constraint(sent, pltpu.VMEM), gain, *weights)


def decode_kernel(
    code_ref, ready_ref, scale_ref, router_ref, peak_buf, even_buf, odd_buf, even_root, odd_root, wide_buf, scale_buf, router_buf, sems
):
    parts = code_ref.shape[0]
    experts, rows, _ = wide_buf.shape
    tiles = rows // 8
    total = experts * rows
    steps = parts // PAIR

    def wide_copy(e):
        return pltpu.make_async_copy(wide_buf.at[e], ready_ref.at[e], sems.at[e])

    scale_copy = pltpu.make_async_copy(scale_buf, scale_ref, sems.at[experts])
    router_copy = pltpu.make_async_copy(router_buf, router_ref, sems.at[experts + 1])

    for s in range(parts):
        router_buf[:, s * LANES : (s + 1) * LANES] = code_ref[s, total + 8 :, :]
        peak_buf[s] = code_ref[s, total : total + 8, :].astype(jnp.float32)
    router_copy.start()

    source = lax.broadcasted_iota(jnp.int32, (parts, PAIR * LANES), 0)
    column = lax.broadcasted_iota(jnp.int32, (parts, PAIR * LANES), 1) // LANES

    def take(e, step, peaks, values, squares):
        first = step * PAIR
        spread = jnp.where(source == column + first, 1.0, 0.0).astype(jnp.bfloat16)
        peak = jnp.dot(peaks, spread, preferred_element_type=jnp.float32)
        for u in range(PAIR):
            code = code_ref[first + u, e * rows : (e + 1) * rows, :].astype(jnp.float32)
            value = jnp.log2(code) * peak[:, u * LANES : (u + 1) * LANES]
            values[first + u] = value
            squares = squares + value * value
        return squares

    def give(e, step, values, roots):
        for u in range(PAIR):
            s = step * PAIR + u
            at = pl.ds(pl.multiple_of(s * LANES, LANES), LANES)
            wide_buf[e, :, at] = (values[s] * roots[...]).astype(jnp.bfloat16)

    lane = lax.broadcasted_iota(jnp.int32, (8, LANES), 1)
    row = lax.broadcasted_iota(jnp.int32, (8, LANES), 0)
    buffers = ((even_buf, even_root), (odd_buf, odd_root))
    for e in range(experts + 1):
        values, roots = buffers[e % 2]
        old_values, old_roots = buffers[1 - e % 2]
        if e < experts:
            peaks = jnp.concatenate([peak_buf[:, 2 * e, :], peak_buf[:, 2 * e + 1, :]], axis=1)
            peaks = peaks.T[:rows].astype(jnp.bfloat16)

        def step(i, squares):
            if e < experts:
                squares = take(e, i, peaks, values, squares)
            if e > 0:
                give(e - 1, i, old_values, old_roots)
            return squares

        squares = lax.fori_loop(0, steps, step, jnp.zeros((rows, LANES), jnp.float32))
        if e > 0:
            wide_copy(e - 1).start()
        if e < experts:
            square = jnp.sum(squares, axis=1, keepdims=True)
            root = lax.rsqrt(square)
            roots[...] = jnp.broadcast_to(root, (rows, LANES))
            scale = square * root * (1.0 / SPAN)
            for first in range(0, tiles, 16):
                line = jnp.zeros((8, LANES), jnp.float32)
                last = min(first + 16, tiles)
                for j in range(first, last):
                    line = jnp.where(lane - row == 8 * (j - first), scale[8 * j : 8 * j + 8], line)
                width = 8 * (last - first)
                scale_buf[e : e + 1, 8 * first : 8 * last] = jnp.sum(line, axis=0, keepdims=True)[:, :width]
        if e == experts - 1:
            scale_copy.start()
    router_copy.wait()
    scale_copy.wait()
    for e in range(experts):
        wide_copy(e).wait()


def decode(code, experts, rows):
    parts, height, _ = code.shape
    total = experts * rows
    hbm = pl.BlockSpec(memory_space=pltpu.HBM)
    tail = height - total - 8
    return pl.pallas_call(
        decode_kernel,
        in_specs=[pl.BlockSpec(memory_space=pltpu.VMEM)],
        out_specs=[hbm] * 3,
        out_shape=[
            jax.ShapeDtypeStruct((experts, rows, parts * LANES), jnp.bfloat16),
            jax.ShapeDtypeStruct((experts, rows), jnp.float32),
            jax.ShapeDtypeStruct((tail, parts * LANES), jnp.bfloat16),
        ],
        scratch_shapes=[
            pltpu.VMEM((parts, 8, LANES), jnp.float32),
            pltpu.VMEM((parts, rows, LANES), jnp.float32),
            pltpu.VMEM((parts, rows, LANES), jnp.float32),
            pltpu.VMEM((rows, LANES), jnp.float32),
            pltpu.VMEM((rows, LANES), jnp.float32),
            pltpu.VMEM((experts, rows, parts * LANES), jnp.bfloat16),
            pltpu.VMEM((experts, rows), jnp.float32),
            pltpu.VMEM((tail, parts * LANES), jnp.bfloat16),
            pltpu.SemaphoreType.DMA((experts + 2,)),
        ],
        compiler_params=pltpu.CompilerParams(vmem_limit_bytes=20 * 2**20),
        name="decode",
    )(pltpu.with_memory_space_constraint(code, pltpu.VMEM))


def of_all_experts(x):
    count = lax.axis_size("expert")
    return [x] + [lax.ppermute(x, "expert", [(i, i ^ j) for i in range(count)]) for j in range(1, count)]


def per_device(train_down, other_down, router_weight, router_gain):
    parts = lax.axis_size("shard")
    experts, length, _ = train_down.shape
    rows = length // parts
    weights = of_all_experts(router_weight.T)
    sent = encode(train_down, other_down, parts, experts * rows + 24)
    sent = with_router(sent, router_gain[None], weights)
    code = lax.all_to_all(sent, "shard", 0, 0, tiled=True)
    ready_down, scale_down, serve_router = decode(code, experts, rows)
    return (ready_down, scale_down, serve_router.T)


def solution(mesh):
    in_specs = (
        P("expert", None, "shard"),
        P("expert", None, "shard"),
        P("shard", "expert"),
        P("shard"),
    )
    out_specs = (P("expert", "shard", None), P("expert", "shard"), P())
    return jax.shard_map(
        per_device, mesh=mesh, in_specs=in_specs, out_specs=out_specs, check_vma=False
    )
```

```python
import jax
import jax.numpy as jnp
from jax import lax
from jax.experimental import pallas as pl
from jax.experimental.pallas import tpu as pltpu
from jax.sharding import PartitionSpec as P


LANES = 128
SPAN = 125.0
FLOOR = 1e-36
TOGETHER = 2


def encode_kernel(train_ref, other_ref, out_ref, train_buf, other_buf, train_sems, other_sems):
    turns, experts, rows, _ = train_buf.shape
    parts, rows = turns * TOGETHER, rows // TOGETHER
    tiles = rows // 8
    place = lax.broadcasted_iota(jnp.int32, (8, LANES), 1) - lax.broadcasted_iota(jnp.int32, (8, LANES), 0)

    def train_copy(d):
        return pltpu.make_async_copy(train_ref.at[:, pl.ds(d * TOGETHER * rows, TOGETHER * rows), :], train_buf.at[d], train_sems.at[d])

    def other_copy(d):
        return pltpu.make_async_copy(other_ref.at[:, pl.ds(d * TOGETHER * rows, TOGETHER * rows), :], other_buf.at[d], other_sems.at[d])

    for d in range(turns):
        train_copy(d).start()
        other_copy(d).start()

    def code_of(i, u):
        d = i * TOGETHER + u
        near = slice(u * rows, (u + 1) * rows)
        peaks = []
        for e in range(0, experts, 2):
            x = jnp.concatenate([train_buf[i, e + h, near] + other_buf[i, e + h, near].astype(jnp.float32) for h in range(2)])
            peak = jnp.max(jnp.abs(x.astype(jnp.bfloat16)), axis=1, keepdims=True)
            peak = jnp.maximum(peak, jnp.bfloat16(FLOOR)).astype(jnp.float32)
            code = jnp.exp2(x * (SPAN / peak))
            out_ref[d, e * rows : (e + 2) * rows, :] = code.astype(jnp.bfloat16)
            for h in range(2):
                for first in (0, 16):
                    line = jnp.zeros((8, LANES), jnp.float32)
                    for k in range(first, min(first + 16, tiles)):
                        at = h * rows + 8 * k
                        line = jnp.where(place == 8 * (k - first), peak[at : at + 8], line)
                    peaks.append(jnp.sum(line, axis=0, keepdims=True))
        out_ref[d, experts * rows : experts * rows + 8, :] = jnp.concatenate(peaks).astype(jnp.bfloat16)

    def step(i, carry):
        train_copy(i).wait()
        other_copy(i).wait()
        for u in range(TOGETHER):
            code_of(i, u)
        return carry

    lax.fori_loop(0, turns, step, 0)


def encode(train, other, parts, height):
    experts, length, _ = train.shape
    rows = length // parts
    hbm = pl.BlockSpec(memory_space=pltpu.HBM)
    return pl.pallas_call(
        encode_kernel,
        in_specs=[hbm, hbm],
        out_specs=pl.BlockSpec(memory_space=pltpu.VMEM),
        out_shape=pltpu.VMEM((parts, height, LANES), jnp.bfloat16),
        scratch_shapes=[
            pltpu.VMEM((parts // TOGETHER, experts, TOGETHER * rows, LANES), jnp.float32),
            pltpu.VMEM((parts // TOGETHER, experts, TOGETHER * rows, LANES), jnp.bfloat16),
            pltpu.SemaphoreType.DMA((parts // TOGETHER,)),
            pltpu.SemaphoreType.DMA((parts // TOGETHER,)),
        ],
        compiler_params=pltpu.CompilerParams(vmem_limit_bytes=22 * 2**20),
        name="encode",
    )(pltpu.with_memory_space_constraint(train, pltpu.HBM), pltpu.with_memory_space_constraint(other, pltpu.HBM))


def router_kernel(sent_ref, gain_ref, w0, w1, w2, w3, out_ref):
    parts, height, _ = out_ref.shape
    mine = lax.axis_index("expert")
    low = jnp.concatenate([w0[...], w1[...]]) * gain_ref[...]
    high = jnp.concatenate([w2[...], w3[...]]) * gain_ref[...]
    low, high = [jnp.where(mine & 1 != 0, pltpu.roll(x, 4, 0), x) for x in (low, high)]
    low, high = jnp.where(mine & 2 != 0, high, low), jnp.where(mine & 2 != 0, low, high)
    both = jnp.concatenate([low, high]).astype(jnp.bfloat16)
    for d in range(parts):
        out_ref[d, height - 16 :, :] = both


def with_router(sent, gain, weights):
    vmem = pl.BlockSpec(memory_space=pltpu.VMEM)
    return pl.pallas_call(
        router_kernel,
        in_specs=[vmem] * (2 + len(weights)),
        out_specs=vmem,
        out_shape=pltpu.VMEM(sent.shape, sent.dtype),
        input_output_aliases={0: 0},
        compiler_params=pltpu.CompilerParams(vmem_limit_bytes=2 * 2**20),
        name="router",
    )(pltpu.with_memory_space_constraint(sent, pltpu.VMEM), gain, *weights)


def decode_kernel(
    code_ref, ready_ref, scale_ref, router_ref, peak_buf, spread_buf, even_buf, odd_buf, even_root, odd_root, wide_buf, scale_buf, router_buf, sems
):
    parts = code_ref.shape[0]
    experts, rows, _ = wide_buf.shape
    total = experts * rows
    stages = [(e, 0, rows) for e in range(experts - 1)] + [(experts - 1, 0, LANES), (experts - 1, LANES, rows)]

    def wide_copy(n):
        e, low, high = stages[n]
        near = pl.ds(low, high - low)
        return pltpu.make_async_copy(wide_buf.at[e, near], ready_ref.at[e, near], sems.at[n])

    scale_copy = pltpu.make_async_copy(scale_buf, scale_ref, sems.at[len(stages)])
    router_copy = pltpu.make_async_copy(router_buf, router_ref, sems.at[len(stages) + 1])

    for s in range(parts):
        router_buf[:, s * LANES : (s + 1) * LANES] = code_ref[s, total + 8 :, :]
        peak_buf[s] = code_ref[s, total : total + 8, :].astype(jnp.float32)
    router_copy.start()

    source = lax.broadcasted_iota(jnp.int32, (parts, parts * LANES), 0)
    column = lax.broadcasted_iota(jnp.int32, (parts, parts * LANES), 1) // LANES
    spread_buf[...] = jnp.where(source == column, 1.0, 0.0).astype(jnp.bfloat16)

    def take(n, values):
        e, low, high = stages[n]
        peaks = jnp.concatenate([peak_buf[:, 2 * e, :], peak_buf[:, 2 * e + 1, :]], axis=1)
        peaks = peaks.T[low:high].astype(jnp.bfloat16)
        peak = jnp.dot(peaks, spread_buf[...], preferred_element_type=jnp.float32)
        squares = jnp.zeros((high - low, LANES), jnp.float32)
        for s in range(parts):
            code = code_ref[s, e * rows + low : e * rows + high, :].astype(jnp.float32)
            value = jnp.log2(code) * peak[:, s * LANES : (s + 1) * LANES]
            values[s, : high - low] = value
            squares = squares + value * value
        return squares

    def give(n, values, roots):
        e, low, high = stages[n]
        for s in range(parts):
            value = values[s, : high - low] * roots[: high - low]
            wide_buf[e, low:high, s * LANES : (s + 1) * LANES] = value.astype(jnp.bfloat16)

    place = lax.broadcasted_iota(jnp.int32, (8, LANES), 1) - lax.broadcasted_iota(jnp.int32, (8, LANES), 0)
    buffers = ((even_buf, even_root), (odd_buf, odd_root))
    for n in range(len(stages) + 1):
        values, roots = buffers[n % 2]
        if n < len(stages):
            squares = take(n, values)
        if n > 0:
            give(n - 1, *buffers[1 - n % 2])
            wide_copy(n - 1).start()
        if n < len(stages):
            e, low, high = stages[n]
            square = jnp.sum(squares, axis=1, keepdims=True)
            root = lax.rsqrt(square)
            roots[: high - low] = jnp.broadcast_to(root, (high - low, LANES))
            scale = square * root * (1.0 / SPAN)
            for first in range(low, high, LANES):
                line = jnp.zeros((8, LANES), jnp.float32)
                last = min(first + LANES, high)
                for at in range(first, last, 8):
                    line = jnp.where(place == at - first, scale[at - low : at - low + 8], line)
                scale_buf[e : e + 1, first:last] = jnp.sum(line, axis=0, keepdims=True)[:, : last - first]
        if n == len(stages) - 1:
            scale_copy.start()
    router_copy.wait()
    scale_copy.wait()
    for n in range(len(stages)):
        wide_copy(n).wait()


def decode(code, experts, rows):
    parts, height, _ = code.shape
    total = experts * rows
    hbm = pl.BlockSpec(memory_space=pltpu.HBM)
    tail = height - total - 8
    return pl.pallas_call(
        decode_kernel,
        in_specs=[pl.BlockSpec(memory_space=pltpu.VMEM)],
        out_specs=[hbm] * 3,
        out_shape=[
            jax.ShapeDtypeStruct((experts, rows, parts * LANES), jnp.bfloat16),
            jax.ShapeDtypeStruct((experts, rows), jnp.float32),
            jax.ShapeDtypeStruct((tail, parts * LANES), jnp.bfloat16),
        ],
        scratch_shapes=[
            pltpu.VMEM((parts, 8, LANES), jnp.float32),
            pltpu.VMEM((parts, parts * LANES), jnp.bfloat16),
            pltpu.VMEM((parts, rows, LANES), jnp.float32),
            pltpu.VMEM((parts, rows, LANES), jnp.float32),
            pltpu.VMEM((rows, LANES), jnp.float32),
            pltpu.VMEM((rows, LANES), jnp.float32),
            pltpu.VMEM((experts, rows, parts * LANES), jnp.bfloat16),
            pltpu.VMEM((experts, rows), jnp.float32),
            pltpu.VMEM((tail, parts * LANES), jnp.bfloat16),
            pltpu.SemaphoreType.DMA((experts + 3,)),
        ],
        compiler_params=pltpu.CompilerParams(vmem_limit_bytes=20 * 2**20),
        name="decode",
    )(pltpu.with_memory_space_constraint(code, pltpu.VMEM))


def of_all_experts(x):
    count = lax.axis_size("expert")
    return [x] + [lax.ppermute(x, "expert", [(i, i ^ j) for i in range(count)]) for j in range(1, count)]


def per_device(train_down, other_down, router_weight, router_gain):
    parts = lax.axis_size("shard")
    experts, length, _ = train_down.shape
    rows = length // parts
    weights = of_all_experts(router_weight.T)
    sent = encode(train_down, other_down, parts, experts * rows + 24)
    sent = with_router(sent, router_gain[None], weights)
    code = lax.all_to_all(sent, "shard", 0, 0, tiled=True)
    ready_down, scale_down, serve_router = decode(code, experts, rows)
    return (ready_down, scale_down, serve_router.T)


def solution(mesh):
    in_specs = (
        P("expert", None, "shard"),
        P("expert", None, "shard"),
        P("shard", "expert"),
        P("shard"),
    )
    out_specs = (P("expert", "shard", None), P("expert", "shard"), P())
    return jax.shard_map(
        per_device, mesh=mesh, in_specs=in_specs, out_specs=out_specs, check_vma=False
    )
```
